32 devices in a mesh: area: 8 (over y, x, core), inarea: 4 (over z).
Axes of the slice: x: 2, y: 2, z: 4, core: 2. Of those that a mesh axis runs over, the one named last changes fastest.
Arguments:
- spikes: int32 [2, 8, 16384], P(None, None, ('area', 'inarea')), may hold values 0 or 1
- release: float32 [8, 16384], P(None, ('area', 'inarea')), may hold values from 0.2 to 1
- potential: float32 [8, 16384], P(None, ('area', 'inarea')), may hold values from -6 to 6
- pre_trace: float32 [8, 16384], P(None, ('area', 'inarea')), may hold values from 0 to 2
- post_trace: float32 [8, 16384], P(None, ('area', 'inarea')), may hold values from 0 to 2
- w_local: float32 [16384, 2048], P(('area', 'inarea')), may hold values from -0.125 to 0.125
- w_long: float32 [16384, 3072], P(('area', 'inarea')), may hold values from -0.109375 to 0.109375
- sources: int32 [8, 12], replicated, may hold values from 0 to 63, as said below
- counts: int32 [8], replicated, may hold values from 512 to 2048, as said below
Outputs:
- voltage: float32 [8, 16384], P(None, ('area', 'inarea'))
- volley: float32 [8, 16384], P(None, ('area', 'inarea'))
- presyn: float32 [8, 16384], P(None, ('area', 'inarea'))
- postsyn: float32 [8, 16384], P(None, ('area', 'inarea'))
- local_new: float32 [16384, 2048], P(('area', 'inarea'))
- long_new: float32 [16384, 3072], P(('area', 'inarea'))
The draws below stay inside these ranges and needn't reach their ends.
Inputs may be any that keep to these rules, and one draw needn't show every extreme that they name: `sources`: no area takes a block of its own; the 12 blocks of one area lie in 12 different runs of 2 blocks that start at multiples of 2. `counts`: some area is full in every draw.
All inputs are finite; a program needn't handle non-finite values. No bound on the sum of `spikes` on one device may be relied on, other than what follows from the above.
Results may differ from the reference program's by a relative error of at most 0.0001.
Values sent between devices are 32-bit elements; how exact they have to be, the bound alone decides.
No kernel may reach another device: no remote copies, remote signals or barrier semaphores. Data moves between devices by JAX's collectives and lax.ppermute only.
A program may use at most 128 MiB of HBM per device.

```python
import jax
import jax.numpy as jnp
from jax import lax

BLOCK = 256
NB_DEV = 2
SLOTS = 12
STEPS = 2
REPEAT_RUNS = 8
CORTICAL_PATCHES = 8
CELLS_PER_PATCH = 2048
NEURONS = 16384


def draw_sources(key, part):
    inner_size = CELLS_PER_PATCH // (NB_DEV * BLOCK)
    others = (CORTICAL_PATCHES - 1) * inner_size
    keys = jax.random.split(jax.random.fold_in(key, 11), CORTICAL_PATCHES)

    def one_area(area_key, area_index):
        order = jax.random.permutation(area_key, others)[:SLOTS].astype(jnp.int32)
        device = order + inner_size * (order >= area_index * inner_size).astype(jnp.int32)
        within = jax.random.randint(jax.random.fold_in(area_key, 7), (SLOTS,), 0, NB_DEV)
        return (device * NB_DEV + within).astype(jnp.int32)
    return jax.vmap(one_area)(keys, jnp.arange(CORTICAL_PATCHES, dtype=jnp.int32))


def draw_counts(key, part):
    base = jax.random.randint(jax.random.fold_in(key, 5), (CORTICAL_PATCHES,), CELLS_PER_PATCH // 4, CELLS_PER_PATCH + 1)
    filled = jax.random.randint(jax.random.fold_in(key, 3), (), 0, CORTICAL_PATCHES)
    return jnp.where(jnp.arange(CORTICAL_PATCHES) == filled, CELLS_PER_PATCH, base).astype(jnp.int32)


def set_ends(array, rng, least, top_value):
    longest = array.shape.index(max(array.shape))
    spots = []
    for shift in (0, 1):
        where = [jax.random.randint(jax.random.fold_in(rng, axis), (), 0, length) for axis, length in enumerate(array.shape)]
        where[longest] = (where[longest] + shift) % array.shape[longest]
        spots.append(tuple(where))
    return array.at[spots[0]].set(least).at[spots[1]].set(top_value)


def shard_levels(rng, extent, cuts, least, high):
    def one(position, blocks):
        steps = jax.random.uniform(jax.random.fold_in(jax.random.fold_in(rng, 6), position), (blocks,), jnp.float32, least / len(cuts), high / len(cuts))
        return jnp.repeat(jnp.exp(steps), extent[position] // blocks).reshape((-1,) + (1,) * (len(extent) - position - 1))

    level = one(*cuts[0])
    for cut in cuts[1:]:
        level = level * one(*cut)
    return level


def gaussian(stream_key, shape, width, bound, cuts=(), kind=jnp.bfloat16):
    drawn = width * jax.random.normal(stream_key, shape, jnp.float32)
    if cuts:
        drawn = drawn * shard_levels(stream_key, shape, cuts, -0.22, 0.18)
    return jnp.clip(drawn, -bound, bound).astype(kind)


def setup_inputs(seed: int = 0) -> dict:
    arg_keys = jax.random.split(jax.random.key(seed), 10)
    return {
        "spikes": set_ends((jax.random.randint(arg_keys[0], (STEPS, REPEAT_RUNS, NEURONS), 0, 2) < 1).astype(jnp.int32), jax.random.fold_in(arg_keys[0], 1), 0, 1),
        "release": jnp.clip(0.2 + 0.8 * jax.random.uniform(arg_keys[1], (REPEAT_RUNS, NEURONS), jnp.float32) ** shard_levels(arg_keys[1], (REPEAT_RUNS, NEURONS), ((1, 32),), -0.2, 0.2), 0.2, 1.0),
        "potential": gaussian(arg_keys[2], (REPEAT_RUNS, NEURONS), 1.0, 6.0, ((1, 32),), jnp.float32),
        "pre_trace": jnp.clip(2.0 * jax.random.uniform(arg_keys[3], (REPEAT_RUNS, NEURONS), jnp.float32) ** shard_levels(arg_keys[3], (REPEAT_RUNS, NEURONS), ((1, 32),), -0.2, 0.2), 0.0, 2.0),
        "post_trace": jnp.clip(2.0 * jax.random.uniform(arg_keys[4], (REPEAT_RUNS, NEURONS), jnp.float32) ** shard_levels(arg_keys[4], (REPEAT_RUNS, NEURONS), ((1, 32),), -0.2, 0.2), 0.0, 2.0),
        "w_local": gaussian(arg_keys[5], (NEURONS, CELLS_PER_PATCH), CELLS_PER_PATCH ** -0.5, 0.125, ((0, 32),), jnp.float32),
        "w_long": gaussian(arg_keys[6], (NEURONS, SLOTS * BLOCK), (SLOTS * BLOCK) ** -0.5, 0.109375, ((0, 32),), jnp.float32),
        "sources": draw_sources(jax.random.fold_in(arg_keys[9], 71), 0),
        "counts": draw_counts(jax.random.fold_in(arg_keys[9], 71), 0),
    }


ceiling_strength = lax.Precision.HIGHEST
pre_decay = 0.8
postsyn_trace_decay = 0.7
leak_factor = 0.9
adaptation_speed = 0.0005
recovery = 0.2
depletion = 0.5


def reference(spikes, release, potential, pre_trace, post_trace, w_local, w_long, sources, counts):
    positions = jnp.arange(CELLS_PER_PATCH, dtype=jnp.int32)
    active_flags = (positions[None, :] < counts[:, None]).reshape(NEURONS).astype(jnp.float32)
    nearby_coupling = w_local.reshape(CORTICAL_PATCHES, CELLS_PER_PATCH, CELLS_PER_PATCH)
    longrange_coupling = w_long.reshape(CORTICAL_PATCHES, CELLS_PER_PATCH, SLOTS * BLOCK)
    volley, presyn, postsyn, voltage = release, pre_trace, post_trace, potential
    for time_step_index in range(STEPS):
        emitted_pulses = spikes[time_step_index].astype(jnp.float32) * active_flags
        spike_activity = emitted_pulses * volley
        presyn = (pre_decay * presyn + spike_activity) * active_flags
        patch_cell_states = spike_activity.reshape(REPEAT_RUNS, CORTICAL_PATCHES, CELLS_PER_PATCH)
        sending_patch_side = presyn.reshape(REPEAT_RUNS, CORTICAL_PATCHES, CELLS_PER_PATCH)
        distal_cell_states = spike_activity.reshape(REPEAT_RUNS, NEURONS // BLOCK, BLOCK)[:, sources].reshape(REPEAT_RUNS, CORTICAL_PATCHES, SLOTS * BLOCK)
        distal_upstream_mark = presyn.reshape(REPEAT_RUNS, NEURONS // BLOCK, BLOCK)[:, sources].reshape(REPEAT_RUNS, CORTICAL_PATCHES, SLOTS * BLOCK)
        emitting_patch = emitted_pulses.reshape(REPEAT_RUNS, CORTICAL_PATCHES, CELLS_PER_PATCH)
        receiving_patch = postsyn.reshape(REPEAT_RUNS, CORTICAL_PATCHES, CELLS_PER_PATCH)
        current = jnp.einsum("tan,amn->tam", patch_cell_states, nearby_coupling, precision=ceiling_strength)
        current = current + jnp.einsum("tan,amn->tam", distal_cell_states, longrange_coupling, precision=ceiling_strength)
        voltage = (leak_factor * voltage + current.reshape(REPEAT_RUNS, NEURONS)) * active_flags
        nearby_coupling = nearby_coupling + adaptation_speed * (jnp.einsum("whk,whf->hkf", emitting_patch, sending_patch_side, precision=ceiling_strength) - jnp.einsum("whk,whf->hkf", receiving_patch, patch_cell_states, precision=ceiling_strength))
        longrange_coupling = longrange_coupling + adaptation_speed * (jnp.einsum("whk,whf->hkf", emitting_patch, distal_upstream_mark, precision=ceiling_strength) - jnp.einsum("whk,whf->hkf", receiving_patch, distal_cell_states, precision=ceiling_strength))
        postsyn = (postsyn_trace_decay * postsyn + emitted_pulses) * active_flags
        volley = volley + recovery * (1.0 - volley) - depletion * spike_activity
    return voltage, volley, presyn, postsyn, nearby_coupling.reshape(NEURONS, CELLS_PER_PATCH), longrange_coupling.reshape(NEURONS, SLOTS * BLOCK)
```

```python
import functools

import jax
import jax.numpy as jnp
from jax import lax
from jax.experimental import pallas as pl
from jax.experimental.pallas import tpu as pltpu
from jax.sharding import PartitionSpec as P

PRE_DECAY = 0.8
POST_DECAY = 0.7
LEAK = 0.9
RATE = 0.0005
RECOVERY = 0.2
DEPLETION = 0.5

F32 = jnp.float32
BF16 = jnp.bfloat16
NT = (((1,), (1,)), ((), ()))
VM = pltpu.VMEM
SM = pltpu.SMEM
HB = pltpu.HBM
UNROLL = 12


def partner(i, k, size):
    if size & (size - 1) == 0:
        return i ^ k, i ^ k
    return (i + size - k) % size, (i + k) % size


def sender_of(src, i, size):
    if size & (size - 1) == 0:
        return src ^ i
    return (i + size - src) % size


def exchange(x, axis, k):
    size = lax.axis_size(axis)
    return lax.ppermute(x, axis, [(i, partner(i, k, size)[1]) for i in range(size)])


def alive_mask(counts_ref, shape):
    live = counts_ref[lax.axis_index("area")] - lax.axis_index("inarea") * shape[-1]
    return (lax.broadcasted_iota(jnp.int32, shape, len(shape) - 1) < live).astype(F32)


def split(x):
    hi = x.astype(BF16)
    return hi, (x - hi.astype(F32)).astype(BF16)


def dynamics(spikes_ref, release_ref, pre_ref, alive):
    f1 = spikes_ref[0].astype(F32) * alive
    f2 = spikes_ref[1].astype(F32) * alive
    v1 = release_ref[...]
    a1 = f1 * v1
    p1 = (PRE_DECAY * pre_ref[...] + a1) * alive
    v2 = v1 + RECOVERY * (1.0 - v1) - DEPLETION * a1
    a2 = f2 * v2
    return f1, f2, a1, p1, v2, a2


def pre_kernel(counts_ref, spikes_ref, release_ref, pre_ref, pay_ref):
    t = release_ref.shape[0]
    alive = alive_mask(counts_ref, release_ref.shape)
    _, _, a1, p1, _, a2 = dynamics(spikes_ref, release_ref, pre_ref, alive)
    pay_ref[0:t] = a1
    pay_ref[t : 2 * t] = a2
    pay_ref[2 * t : 3 * t] = p1


def prep_kernel(
    per_dev, counts_ref, sources_ref, spikes_ref, release_ref, pre_ref, post_ref, w_hbm,
    which_ref, left_ref, fq_ref, volley_ref, presyn_ref, postsyn_ref, win, wsp, isem,
):
    t, n = release_ref.shape
    tiles, _, block = win.shape
    areas, inner = which_ref.shape
    slots = sources_ref.shape[1]
    area, z = lax.axis_index("area"), lax.axis_index("inarea")

    def fetch(c):
        return pltpu.make_async_copy(w_hbm.at[:, cols_of(c, block)], win.at[c], isem.at[c])

    for c in range(tiles):
        fetch(c).start()

    for k in range(inner):
        first = (area * inner + partner(z, k, inner)[0]) * per_dev

        @pl.loop(0, areas)
        def _(b):
            which = jnp.int32(0)
            for s in range(slots):
                off = sources_ref[b, s] - first
                which = which + jnp.where((off >= 0) & (off < per_dev), off, 0)
            which_ref[b, k] = which

    alive = alive_mask(counts_ref, release_ref.shape)
    f1, f2, a1, p1, v2, a2 = dynamics(spikes_ref, release_ref, pre_ref, alive)
    q1 = post_ref[...]
    q2 = (POST_DECAY * q1 + f1) * alive
    volley_ref[...] = v2 + RECOVERY * (1.0 - v2) - DEPLETION * a2
    presyn_ref[...] = (PRE_DECAY * p1 + a2) * alive
    postsyn_ref[...] = (POST_DECAY * q2 + f2) * alive
    fq_ref[...] = jnp.concatenate([f1, -q1], 0)
    factor = RATE * jnp.concatenate([-q1, f2 - q2, f1 + PRE_DECAY * f2], 0)
    fh = factor.astype(BF16).astype(F32)
    pad = left_ref.shape[1] - 9 * t
    left = jnp.concatenate([fh, fh, factor - fh, jnp.zeros((pad, n), F32)], 0)
    left_ref[...] = left.T.astype(BF16)

    @pl.loop(0, tiles)
    def _(c):
        fetch(c).wait()
        hi, lo = split(win[c])
        wsp[c, :, 0:block] = hi
        wsp[c, :, block : 2 * block] = lo


def mid_kernel(which_ref, *refs):
    areas, inner = which_ref.shape
    shared, outs = refs[:inner], refs[inner:]
    block = outs[0].shape[-1]
    area = lax.axis_index("area")
    for h in range(1, areas):
        to = partner(area, h, areas)[1]
        for k in range(inner):
            start = pl.multiple_of(which_ref[to, k] * block, block)
            outs[h - 1][k] = shared[k][:, pl.ds(start, block)]


def cols_of(c, block):
    return pl.ds(pl.multiple_of(c * block, block), block)


def tile_terms(z, t):
    a1, a2, p1 = z[0:t], z[t : 2 * t], z[2 * t : 3 * t]
    zh = z.astype(BF16).astype(F32)
    zl = z - zh
    right = jnp.concatenate([zh, zl, zh, jnp.zeros((t, z.shape[1]), F32)], 0).astype(BF16)
    x = LEAK * a1 + a2
    xh = x.astype(BF16).astype(F32)
    drive = jnp.concatenate([xh, x - xh], 0).astype(BF16)
    late = jnp.concatenate([zh[t : 2 * t], zl[t : 2 * t]], 0).astype(BF16)
    th, tl = split(jnp.concatenate([p1, a1], 0))
    return (
        right,
        jnp.concatenate([drive, drive], 1),
        jnp.concatenate([late, late], 1),
        jnp.concatenate([th, tl], 1),
    )


def tile_step(w, halves, z, left, t, sum_ref, gram_ref):
    right, drive, late, traces = tile_terms(z, t)
    sum_ref[...] += lax.dot_general(drive, halves, NT, preferred_element_type=F32)
    gram_ref[...] += lax.dot_general(late, traces, NT, preferred_element_type=F32)
    return w + jnp.dot(left, right, preferred_element_type=F32)


def near_kernel(left_ref, w_hbm, *refs):
    inner = len(refs) - 7
    shared = refs[:inner]
    new_hbm, sum_ref, gram_ref, win, wout, isem, osem = refs[inner:]
    t = sum_ref.shape[0] // 2
    tiles, n, block = win.shape
    z = lax.axis_index("inarea")
    per = tiles // inner

    def fetch(c):
        return pltpu.make_async_copy(w_hbm.at[:, cols_of(c, block)], win.at[c], isem.at[c])

    def flush(c):
        return pltpu.make_async_copy(wout.at[c], new_hbm.at[:, cols_of(c, block)], osem.at[c])

    def tile_of(k, h):
        return partner(z, k, inner)[0] * per + h

    for k in range(inner):
        for h in range(per):
            fetch(tile_of(k, h)).start()
    sum_ref[...] = jnp.zeros_like(sum_ref)
    gram_ref[...] = jnp.zeros_like(gram_ref)
    for k in range(inner):

        @pl.loop(0, per)
        def _(h):
            c = tile_of(k, h)
            fetch(c).wait()
            w = win[c]
            wout[c] = tile_step(
                w, jnp.concatenate(split(w), 1), shared[k][:, cols_of(h, block)],
                left_ref[:, 0 : 10 * t], t, sum_ref, gram_ref)
            flush(c).start()

    for c in range(tiles):
        flush(c).wait()


def far_kernel(
    per_dev, counts_ref, sources_ref, potential_ref, fq_ref, left_ref, sum_ref, gram_ref,
    win, wsp, *refs,
):
    *fars, new_hbm, voltage_ref, wout, osem, total, gram, far_ref = refs
    t, n = potential_ref.shape
    slots, _, block = win.shape
    areas, inner = len(fars) + 1, far_ref.shape[1]
    area, z = lax.axis_index("area"), lax.axis_index("inarea")

    def flush(c):
        return pltpu.make_async_copy(wout.at[c], new_hbm.at[:, cols_of(c, block)], osem.at[c])

    for h in range(1, areas):
        far_ref[partner(area, h, areas)[0]] = fars[h - 1][...]
    total[...] = sum_ref[...]
    gram[...] = gram_ref[...]

    @pl.loop(0, slots, unroll=UNROLL)
    def _(c):
        dev = lax.div(sources_ref[area, c], per_dev)
        k = sender_of(lax.rem(dev, inner), z, inner)
        wout[c] = tile_step(
            win[c], wsp[c], far_ref[lax.div(dev, inner), k], left_ref[:, 0 : 10 * t], t,
            total, gram)
        flush(c).start()

    pairs = gram[0:t] + gram[t : 2 * t]
    drift = jnp.dot(pairs, fq_ref[...], precision=lax.Precision.HIGHEST, preferred_element_type=F32)
    alive = alive_mask(counts_ref, potential_ref.shape)
    voltage_ref[...] = alive * (
        LEAK * LEAK * potential_ref[...] + (total[0:t] + total[t : 2 * t]) + RATE * drift
    )
    for c in range(slots):
        flush(c).wait()


def full(space):
    return pl.BlockSpec(memory_space=space)


def local(spikes, release, potential, pre_trace, post_trace, w_local, w_long, sources, counts):
    t, n = release.shape
    slots = sources.shape[1]
    block = w_long.shape[1] // slots
    per_dev = n // block
    areas = lax.axis_size("area")
    inner = lax.axis_size("inarea")
    tiles = w_local.shape[1] // block
    like = jax.ShapeDtypeStruct

    def hb(*xs):
        return [pltpu.with_memory_space_constraint(x, HB) for x in xs]

    def vm(*xs):
        return [pltpu.with_memory_space_constraint(x, VM) for x in xs]

    def params(mib):
        return pltpu.CompilerParams(vmem_limit_bytes=mib << 20)

    pay = pl.pallas_call(
        pre_kernel,
        out_shape=VM((3 * t, n), F32),
        in_specs=[full(SM)] + [full(VM)] * 3,
        out_specs=full(VM),
        compiler_params=params(2),
        name="pre",
    )(*hb(counts, spikes, release, pre_trace))

    shared = [pay] + [
        exchange(pay, "inarea", k) for k in range(1, inner)
    ]

    which, left, fq, volley, presyn, postsyn, tiles_w, halves_w = pl.pallas_call(
        functools.partial(prep_kernel, per_dev),
        out_shape=(
            SM((areas, inner), jnp.int32),
            VM((n, 128), BF16),
            VM((2 * t, n), F32),
            like((t, n), F32),
            like((t, n), F32),
            like((t, n), F32),
            VM((slots, n, block), F32),
            VM((slots, n, 2 * block), BF16),
        ),
        in_specs=[full(SM)] * 2 + [full(VM)] * 4 + [full(HB)],
        out_specs=(full(SM),) + (full(VM),) * 7,
        scratch_shapes=[pltpu.SemaphoreType.DMA((slots,))],
        compiler_params=params(4),
        cost_estimate=pl.CostEstimate(
            flops=2 * n * w_long.shape[1] * 512, bytes_accessed=8 * w_long.size, transcendentals=0),
        name="prep",
    )(*hb(counts, sources, spikes, release, pre_trace, post_trace, w_long))

    sends = pl.pallas_call(
        mid_kernel,
        out_shape=(VM((inner, 3 * t, block), F32),) * (areas - 1),
        in_specs=[full(SM)] + [full(VM)] * inner,
        out_specs=(full(VM),) * (areas - 1),
        compiler_params=params(2 + areas * inner * 12 * t * block // (1 << 20)),
        name="mid",
    )(which, *shared)
    fars = [exchange(x, "area", h + 1) for h, x in enumerate(sends)]

    local_new, sums, grams = pl.pallas_call(
        near_kernel,
        out_shape=(
            HB(w_local.shape, F32),
            VM((2 * t, n), F32),
            VM((2 * t, 2 * t), F32),
        ),
        in_specs=[full(VM), full(HB)] + [full(VM)] * inner,
        out_specs=(full(HB),) + (full(VM),) * 2,
        scratch_shapes=[
            VM((tiles, n, block), F32),
            VM((tiles, n, block), F32),
            pltpu.SemaphoreType.DMA((tiles,)),
            pltpu.SemaphoreType.DMA((tiles,)),
        ],
        compiler_params=params(14),
        cost_estimate=pl.CostEstimate(
            flops=2 * n * w_local.shape[1] * 512, bytes_accessed=8 * w_local.size, transcendentals=0),
        name="near",
    )(*vm(left), *hb(w_local), *shared)

    long_new, voltage = pl.pallas_call(
        functools.partial(far_kernel, per_dev),
        out_shape=(HB(w_long.shape, F32), like((t, n), F32)),
        in_specs=[full(SM)] * 2 + [full(VM)] * (6 + areas),
        out_specs=(full(HB), full(VM)),
        scratch_shapes=[
            VM((slots, n, block), F32),
            pltpu.SemaphoreType.DMA((slots,)),
            VM((2 * t, n), F32),
            VM((2 * t, 2 * t), F32),
            VM((areas, inner, 3 * t, block), F32),
        ],
        compiler_params=params(12 + areas * inner * 12 * t * block // (1 << 20)),
        cost_estimate=pl.CostEstimate(
            flops=2 * n * w_long.shape[1] * 512, bytes_accessed=8 * w_long.size, transcendentals=0),
        name="far",
    )(*hb(counts, sources, potential), *vm(fq, left, sums, grams, tiles_w, halves_w), *fars)
    return voltage, volley, presyn, postsyn, local_new, long_new


def solution(mesh):
    split_last = P(None, ("area", "inarea"))
    rows = P(("area", "inarea"), None)
    return jax.shard_map(
        local,
        mesh=mesh,
        in_specs=(
            P(None, None, ("area", "inarea")),
            split_last, split_last, split_last, split_last, rows, rows, P(), P(),
        ),
        out_specs=(split_last, split_last, split_last, split_last, rows, rows),
        check_vma=False,
    )
```

```python
import functools

import jax
import jax.numpy as jnp
from jax import lax
from jax.experimental import pallas as pl
from jax.experimental.pallas import tpu as pltpu
from jax.sharding import PartitionSpec as P

PRE_DECAY = 0.8
POST_DECAY = 0.7
LEAK = 0.9
RATE = 0.0005
RECOVERY = 0.2
DEPLETION = 0.5

F32 = jnp.float32
BF16 = jnp.bfloat16
NT = (((1,), (1,)), ((), ()))
VM = pltpu.VMEM
SM = pltpu.SMEM
HB = pltpu.HBM
AORDER = (6, 2, 1, 4, 7, 3, 5)
EARLY = 3


def partner(i, k, size):
    if size & (size - 1) == 0:
        return i ^ k, i ^ k
    return (i + size - k) % size, (i + k) % size


def sender_of(src, i, size):
    if size & (size - 1) == 0:
        return src ^ i
    return (i + size - src) % size


def area_order(size):
    if size == 8:
        return AORDER, EARLY
    return tuple(range(1, size)), size // 2


def is_early(k, size):
    order, count = area_order(size)
    early = k == order[0]
    for h in order[1:count]:
        early = early | (k == h)
    return early


def exchange(x, axis, k):
    size = lax.axis_size(axis)
    return lax.ppermute(x, axis, [(i, partner(i, k, size)[1]) for i in range(size)])


def alive_mask(counts_ref, shape):
    live = counts_ref[lax.axis_index("area")] - lax.axis_index("inarea") * shape[-1]
    return (lax.broadcasted_iota(jnp.int32, shape, len(shape) - 1) < live).astype(F32)


def split(x):
    hi = x.astype(BF16)
    return hi, (x - hi.astype(F32)).astype(BF16)


def pre_kernel(
    counts_ref, sources_ref, spikes_ref, release_ref, pre_ref, pay_ref, keep_ref, held_ref
):
    t = release_ref.shape[0]
    alive = alive_mask(counts_ref, release_ref.shape)
    f1 = spikes_ref[0].astype(F32) * alive
    f2 = spikes_ref[1].astype(F32) * alive
    v1 = release_ref[...]
    a1 = f1 * v1
    v2 = v1 + RECOVERY * (1.0 - v1) - DEPLETION * a1
    pay_ref[0:t] = a1
    pay_ref[t : 2 * t] = f2 * v2
    pay_ref[2 * t : 3 * t] = (PRE_DECAY * pre_ref[...] + a1) * alive
    for i, part in enumerate((f1, f2, v2, alive)):
        keep_ref[i * t : (i + 1) * t] = part
    for b in range(sources_ref.shape[0]):
        for c in range(sources_ref.shape[1]):
            held_ref[b, c] = sources_ref[b, c]


def prep_kernel(
    per_dev, sources_ref, pay_ref, keep_ref, w_ref, post_hbm, potential_hbm,
    which_ref, slot_ref, left_ref, fq_ref, base_ref, ends_ref, win, wsp,
    post_ref, potential_ref, msem,
):
    t, n = post_ref.shape
    tiles, _, block = win.shape
    areas, inner = which_ref.shape
    slots = sources_ref.shape[1]
    area, z = lax.axis_index("area"), lax.axis_index("inarea")

    small = [
        pltpu.make_async_copy(post_hbm, post_ref, msem.at[0]),
        pltpu.make_async_copy(potential_hbm, potential_ref, msem.at[1]),
    ]
    for copy in small:
        copy.start()

    for k in range(inner):
        first = (area * inner + partner(z, k, inner)[0]) * per_dev

        @pl.loop(0, areas)
        def _(b):
            which = jnp.int32(0)
            for s in range(slots):
                off = sources_ref[b, s] - first
                which = which + jnp.where((off >= 0) & (off < per_dev), off, 0)
            which_ref[b, k] = which

    first, last = jnp.int32(0), jnp.int32(slots - 1)
    for s in range(slots):
        dev = lax.div(sources_ref[area, s], per_dev)
        origin = lax.div(dev, inner)
        early = is_early(sender_of(origin, area, areas), areas)
        at = jnp.where(early, first, last)
        slot_ref[0, at] = origin
        slot_ref[1, at] = sender_of(lax.rem(dev, inner), z, inner)
        slot_ref[2, at] = jnp.int32(s)
        first = first + jnp.where(early, 1, 0)
        last = last - jnp.where(early, 0, 1)
    slot_ref[3, 0] = first

    for copy in small:
        copy.wait()
    f1, f2, v2, alive = (keep_ref[i * t : (i + 1) * t] for i in range(4))
    a2, p1 = pay_ref[t : 2 * t], pay_ref[2 * t : 3 * t]
    q1 = post_ref[...]
    q2 = (POST_DECAY * q1 + f1) * alive
    ends_ref[0:t] = v2 + RECOVERY * (1.0 - v2) - DEPLETION * a2
    ends_ref[t : 2 * t] = (PRE_DECAY * p1 + a2) * alive
    ends_ref[2 * t : 3 * t] = (POST_DECAY * q2 + f2) * alive
    base_ref[0:t] = alive
    base_ref[t : 2 * t] = LEAK * LEAK * potential_ref[...] * alive
    fq_ref[...] = RATE * jnp.concatenate([f1, -q1], 0)
    factor = RATE * jnp.concatenate([-q1, f2 - q2, f1 + PRE_DECAY * f2], 0)
    fh = factor.astype(BF16).astype(F32)
    pad = left_ref.shape[1] - 9 * t
    left = jnp.concatenate([fh, fh, factor - fh, jnp.zeros((pad, n), F32)], 0)
    left_ref[...] = left.T.astype(BF16)

    @pl.loop(0, tiles)
    def _(c):
        w = w_ref[:, cols_of(c, block)]
        win[c] = w
        hi, lo = split(w)
        wsp[c, :, 0:block] = hi
        wsp[c, :, block : 2 * block] = lo


def mid_kernel(which_ref, *refs):
    areas, inner = which_ref.shape
    shared, outs = refs[:inner], refs[inner:]
    block = outs[0].shape[-1]
    area = lax.axis_index("area")
    for h in range(1, areas):
        to = partner(area, h, areas)[1]
        for k in range(inner):
            start = pl.multiple_of(which_ref[to, k] * block, block)
            outs[h - 1][k] = shared[k][:, pl.ds(start, block)]


def cols_of(c, block):
    return pl.ds(pl.multiple_of(c * block, block), block)


def update_terms(z):
    zh = z.astype(BF16).astype(F32)
    pad = jnp.zeros((z.shape[0] // 3, z.shape[1]), F32)
    return jnp.concatenate([zh, z - zh, zh, pad], 0).astype(BF16)


def current_terms(z, t):
    a1, a2, p1 = z[0:t], z[t : 2 * t], z[2 * t : 3 * t]
    rows = jnp.concatenate([LEAK * a1 + a2, a2], 0)
    rh = rows.astype(BF16).astype(F32)
    rl = rows - rh
    drive = jnp.concatenate([rh[0:t], rl[0:t]], 0).astype(BF16)
    late = jnp.concatenate([rh[t : 2 * t], rl[t : 2 * t]], 0).astype(BF16)
    th, tl = split(jnp.concatenate([p1, a1], 0))
    return (
        jnp.concatenate([drive, drive], 1),
        jnp.concatenate([late, late], 1),
        jnp.concatenate([th, tl], 1),
    )


def dot_nt(x, y):
    return lax.dot_general(x, y, NT, preferred_element_type=F32)


def near_kernel(left_ref, ends_ref, w_ref, *refs):
    inner = len(refs) - 9
    shared = refs[:inner]
    new_hbm, *end_hbm, sum_ref, gram_ref, wout, osem, esem = refs[inner:]
    t = sum_ref.shape[0] // 2
    tiles, n, block = wout.shape
    z = lax.axis_index("inarea")
    per = tiles // inner

    def flush(c):
        return pltpu.make_async_copy(wout.at[c], new_hbm.at[:, cols_of(c, block)], osem.at[c])

    def tile_of(k, h):
        return partner(z, k, inner)[0] * per + h

    ends = [
        pltpu.make_async_copy(ends_ref.at[i * t : (i + 1) * t], ref, esem.at[i])
        for i, ref in enumerate(end_hbm)
    ]
    for copy in ends:
        copy.start()
    total, gram = jnp.zeros(sum_ref.shape, F32), jnp.zeros(gram_ref.shape, F32)
    for k in range(inner):
        for h in range(per):
            c = tile_of(k, h)
            w = w_ref[:, cols_of(c, block)]
            x = shared[k][:, h * block : (h + 1) * block]
            drive, late, traces = current_terms(x, t)
            total = total + dot_nt(drive, jnp.concatenate(split(w), 1))
            gram = gram + dot_nt(late, traces)
            wout[c] = w + jnp.dot(
                left_ref[:, 0 : 10 * t], update_terms(x), preferred_element_type=F32)
            flush(c).start()
    sum_ref[...] = total
    gram_ref[...] = gram

    for c in range(tiles):
        flush(c).wait()
    for copy in ends:
        copy.wait()


def far_tiles(lo, hi, areas, slot_ref, left_ref, win, wsp, blocks, new_hbm, far_ref, wout, osem,
              total, gram):
    t = total.shape[0] // 2
    block = win.shape[2]
    area = lax.axis_index("area")

    def flush(c):
        return pltpu.make_async_copy(wout.at[c], new_hbm.at[:, cols_of(c, block)], osem.at[c])

    for h, ref in blocks:
        far_ref[partner(area, h, areas)[0]] = ref[...]

    def group(places):
        parts, grams = [], []
        for i in places:
            c = slot_ref[2, i]
            z = far_ref[slot_ref[0, i], slot_ref[1, i]]
            wout[c] = win[c] + jnp.dot(
                left_ref[:, 0 : 10 * t], update_terms(z), preferred_element_type=F32)
            drive, late, traces = current_terms(z, t)
            parts.append(dot_nt(drive, wsp[c]))
            grams.append(dot_nt(late, traces))
        total[...] += sum(parts)
        gram[...] += sum(grams)
        for i in places:
            flush(slot_ref[2, i]).start()

    pairs = lax.div(hi - lo, 2)

    @pl.loop(0, pairs)
    def _(i):
        group((lo + 2 * i, lo + 2 * i + 1))

    @pl.when(hi - lo > 2 * pairs)
    def _():
        group((hi - 1,))

    def drain():
        @pl.loop(lo, hi)
        def _(i):
            flush(slot_ref[2, i]).wait()

    return drain


def early_kernel(areas, slot_ref, left_ref, sum_ref, gram_ref, win, wsp, *refs):
    *fars, new_hbm, total, gram, wout, far_ref, osem = refs
    total[...] = sum_ref[...]
    gram[...] = gram_ref[...]
    order, count = area_order(areas)
    blocks = list(zip(order[:count], fars, strict=True))
    far_tiles(0, slot_ref[3, 0], areas, slot_ref, left_ref, win, wsp, blocks, new_hbm, far_ref,
              wout, osem, total, gram)()


def late_kernel(areas, slot_ref, base_ref, fq_ref, left_ref, sum_ref, gram_ref, win, wsp, *refs):
    *fars, _, new_hbm, voltage_hbm, total, gram, wout, vout, far_ref, osem, vsem = refs
    t = vout.shape[0]
    total[...] = sum_ref[...]
    gram[...] = gram_ref[...]
    order, count = area_order(areas)
    blocks = list(zip(order[count:], fars, strict=True))
    drain = far_tiles(slot_ref[3, 0], win.shape[0], areas, slot_ref, left_ref, win, wsp, blocks,
                      new_hbm, far_ref, wout, osem, total, gram)
    pairs = gram[0:t] + gram[t : 2 * t]
    drift = jnp.dot(pairs, fq_ref[...], precision=lax.Precision.HIGHEST, preferred_element_type=F32)
    vout[...] = base_ref[t : 2 * t] + base_ref[0:t] * (total[0:t] + total[t : 2 * t] + drift)
    done = pltpu.make_async_copy(vout, voltage_hbm, vsem)
    done.start()
    drain()
    done.wait()


def full(space):
    return pl.BlockSpec(memory_space=space)


def local(spikes, release, potential, pre_trace, post_trace, w_local, w_long, sources, counts):
    t, n = release.shape
    slots = sources.shape[1]
    block = w_long.shape[1] // slots
    per_dev = n // block
    areas = lax.axis_size("area")
    inner = lax.axis_size("inarea")
    tiles = w_local.shape[1] // block
    cover = pl.CostEstimate(flops=5 * 10**9, bytes_accessed=1 << 24, transcendentals=0)

    def hb(*xs):
        return [pltpu.with_memory_space_constraint(x, HB) for x in xs]

    def vm(*xs):
        return [pltpu.with_memory_space_constraint(x, VM) for x in xs]

    def params(mib):
        return pltpu.CompilerParams(vmem_limit_bytes=mib << 20)

    pay, keep, held = pl.pallas_call(
        pre_kernel,
        out_shape=(
            VM((3 * t, n), F32), VM((4 * t, n), F32), SM(sources.shape, jnp.int32)),
        in_specs=[full(SM)] * 2 + [full(VM)] * 3,
        out_specs=(full(VM),) * 2 + (full(SM),),
        compiler_params=params(2),
        cost_estimate=cover,
        name="pre",
    )(*hb(counts, sources, spikes, release, pre_trace))

    shared = [pay] + [
        exchange(pay, "inarea", k) for k in range(1, inner)
    ]

    which, slot, left, fq, base, ends, tiles_w, halves_w = pl.pallas_call(
        functools.partial(prep_kernel, per_dev),
        out_shape=(
            SM((areas, inner), jnp.int32),
            SM((4, slots), jnp.int32),
            VM((n, 128), BF16),
            VM((2 * t, n), F32),
            VM((2 * t, n), F32),
            VM((3 * t, n), F32),
            VM((slots, n, block), F32),
            VM((slots, n, 2 * block), BF16),
        ),
        in_specs=[full(SM)] + [full(VM)] * 3 + [full(HB)] * 2,
        out_specs=(full(SM),) * 2 + (full(VM),) * 6,
        scratch_shapes=[
            VM((t, n), F32),
            VM((t, n), F32),
            pltpu.SemaphoreType.DMA((2,)),
        ],
        compiler_params=params(4),
        cost_estimate=pl.CostEstimate(
            flops=2 * n * w_long.shape[1] * 512, bytes_accessed=8 * w_long.size, transcendentals=0),
        name="prep",
    )(held, *vm(pay, keep, w_long), *hb(post_trace, potential))

    sends = pl.pallas_call(
        mid_kernel,
        out_shape=(VM((inner, 3 * t, block), F32),) * (areas - 1),
        in_specs=[full(SM)] + [full(VM)] * inner,
        out_specs=(full(VM),) * (areas - 1),
        compiler_params=params(2 + areas * inner * 12 * t * block // (1 << 20)),
        cost_estimate=cover,
        name="mid",
    )(which, *shared)
    order, count = area_order(areas)
    fars = [exchange(sends[h - 1], "area", h) for h in order]

    local_new, volley, presyn, postsyn, sums, grams = pl.pallas_call(
        near_kernel,
        out_shape=(
            HB(w_local.shape, F32),
            *(HB((t, n), F32),) * 3,
            VM((2 * t, n), F32),
            VM((2 * t, 2 * t), F32),
        ),
        in_specs=[full(VM)] * (3 + inner),
        out_specs=(full(HB),) * 4 + (full(VM),) * 2,
        scratch_shapes=[
            VM((tiles, n, block), F32),
            pltpu.SemaphoreType.DMA((tiles,)),
            pltpu.SemaphoreType.DMA((3,)),
        ],
        compiler_params=params(14),
        cost_estimate=pl.CostEstimate(
            flops=2 * n * w_local.shape[1] * 512, bytes_accessed=8 * w_local.size, transcendentals=0),
        name="near",
    )(*vm(left, ends, w_local), *shared)

    far_scratch = [
        VM((slots, n, block), F32),
        VM((areas, inner, 3 * t, block), F32),
        pltpu.SemaphoreType.DMA((slots,)),
    ]
    far_params = params(12 + areas * inner * 12 * t * block // (1 << 20))
    far_cost = pl.CostEstimate(
        flops=n * w_long.shape[1] * 512, bytes_accessed=4 * w_long.size, transcendentals=0)
    soon, then = fars[:count], fars[count:]
    long_new, sums, grams = pl.pallas_call(
        functools.partial(early_kernel, areas),
        out_shape=(HB(w_long.shape, F32), VM((2 * t, n), F32), VM((2 * t, 2 * t), F32)),
        in_specs=[full(SM)] + [full(VM)] * (5 + len(soon)),
        out_specs=(full(HB), full(VM), full(VM)),
        scratch_shapes=far_scratch,
        compiler_params=far_params,
        cost_estimate=far_cost,
        name="early",
    )(slot, *vm(left, sums, grams, tiles_w, halves_w), *soon)

    long_new, voltage = pl.pallas_call(
        functools.partial(late_kernel, areas),
        out_shape=(HB(w_long.shape, F32), HB((t, n), F32)),
        in_specs=[full(SM)] + [full(VM)] * (7 + len(then)) + [full(HB)],
        out_specs=(full(HB),) * 2,
        scratch_shapes=[VM((2 * t, n), F32), VM((2 * t, 2 * t), F32), far_scratch[0], VM((t, n), F32)]
        + far_scratch[1:] + [pltpu.SemaphoreType.DMA],
        input_output_aliases={8 + len(then): 0},
        compiler_params=far_params,
        cost_estimate=far_cost,
        name="late",
    )(slot, *vm(base, fq, left, sums, grams, tiles_w, halves_w), *then, *hb(long_new))
    return voltage, volley, presyn, postsyn, local_new, long_new


def solution(mesh):
    split_last = P(None, ("area", "inarea"))
    rows = P(("area", "inarea"), None)
    return jax.shard_map(
        local,
        mesh=mesh,
        in_specs=(
            P(None, None, ("area", "inarea")),
            split_last, split_last, split_last, split_last, rows, rows, P(), P(),
        ),
        out_specs=(split_last, split_last, split_last, split_last, rows, rows),
        check_vma=False,
    )
```

```python
import functools

import jax
import jax.numpy as jnp
from jax import lax
from jax.experimental import pallas as pl
from jax.experimental.pallas import tpu as pltpu
from jax.sharding import PartitionSpec as P

PRE_DECAY = 0.8
POST_DECAY = 0.7
LEAK = 0.9
RATE = 0.0005
RECOVERY = 0.2
DEPLETION = 0.5

F32 = jnp.float32
BF16 = jnp.bfloat16
NT = (((1,), (1,)), ((), ()))
VM = pltpu.VMEM
SM = pltpu.SMEM
HB = pltpu.HBM
AORDER = (6, 4, 2, 1, 7, 5, 3)
EARLY = 4


def partner(i, k, size):
    if size & (size - 1) == 0:
        return i ^ k, i ^ k
    return (i + size - k) % size, (i + k) % size


def sender_of(src, i, size):
    if size & (size - 1) == 0:
        return src ^ i
    return (i + size - src) % size


def area_order(size):
    if size == 8:
        return AORDER, EARLY
    return tuple(range(1, size)), size // 2


def is_early(k, size):
    order, count = area_order(size)
    early = k == order[0]
    for h in order[1:count]:
        early = early | (k == h)
    return early


def exchange(x, axis, k):
    size = lax.axis_size(axis)
    return lax.ppermute(x, axis, [(i, partner(i, k, size)[1]) for i in range(size)])


def alive_mask(counts_ref, shape):
    live = counts_ref[lax.axis_index("area")] - lax.axis_index("inarea") * shape[-1]
    return (lax.broadcasted_iota(jnp.int32, shape, len(shape) - 1) < live).astype(F32)


def split(x):
    hi = x.astype(BF16)
    return hi, (x - hi.astype(F32)).astype(BF16)


def pre_kernel(
    counts_ref, sources_ref, spikes_ref, release_ref, pre_ref, pay_ref, keep_ref, held_ref
):
    t = release_ref.shape[0]
    alive = alive_mask(counts_ref, release_ref.shape)
    f1 = spikes_ref[0].astype(F32) * alive
    f2 = spikes_ref[1].astype(F32) * alive
    v1 = release_ref[...]
    a1 = f1 * v1
    v2 = v1 + RECOVERY * (1.0 - v1) - DEPLETION * a1
    pay_ref[0:t] = a1
    pay_ref[t : 2 * t] = f2 * v2
    pay_ref[2 * t : 3 * t] = (PRE_DECAY * pre_ref[...] + a1) * alive
    for i, part in enumerate((f1, f2, v2, alive)):
        keep_ref[i * t : (i + 1) * t] = part
    for b in range(sources_ref.shape[0]):
        for c in range(sources_ref.shape[1]):
            held_ref[b, c] = sources_ref[b, c]


def prep_kernel(
    per_dev, sources_ref, pay_ref, keep_ref, w_ref, post_hbm, potential_hbm,
    which_ref, slot_ref, left_ref, fq_ref, base_ref, ends_ref, win, wsp,
    post_ref, potential_ref, msem,
):
    t, n = post_ref.shape
    tiles, _, block = win.shape
    areas, inner = which_ref.shape
    slots = sources_ref.shape[1]
    area, z = lax.axis_index("area"), lax.axis_index("inarea")

    small = [
        pltpu.make_async_copy(post_hbm, post_ref, msem.at[0]),
        pltpu.make_async_copy(potential_hbm, potential_ref, msem.at[1]),
    ]
    for copy in small:
        copy.start()

    for k in range(inner):
        first = (area * inner + partner(z, k, inner)[0]) * per_dev

        @pl.loop(0, areas)
        def _(b):
            which = jnp.int32(0)
            for s in range(slots):
                off = sources_ref[b, s] - first
                which = which + jnp.where((off >= 0) & (off < per_dev), off, 0)
            which_ref[b, k] = which

    first, last = jnp.int32(0), jnp.int32(slots - 1)
    for s in range(slots):
        dev = lax.div(sources_ref[area, s], per_dev)
        origin = lax.div(dev, inner)
        early = is_early(sender_of(origin, area, areas), areas)
        at = jnp.where(early, first, last)
        slot_ref[0, at] = origin
        slot_ref[1, at] = sender_of(lax.rem(dev, inner), z, inner)
        slot_ref[2, at] = jnp.int32(s)
        first = first + jnp.where(early, 1, 0)
        last = last - jnp.where(early, 0, 1)
    slot_ref[3, 0] = first

    for copy in small:
        copy.wait()
    f1, f2, v2, alive = (keep_ref[i * t : (i + 1) * t] for i in range(4))
    a2, p1 = pay_ref[t : 2 * t], pay_ref[2 * t : 3 * t]
    q1 = post_ref[...]
    q2 = (POST_DECAY * q1 + f1) * alive
    ends_ref[0:t] = v2 + RECOVERY * (1.0 - v2) - DEPLETION * a2
    ends_ref[t : 2 * t] = (PRE_DECAY * p1 + a2) * alive
    ends_ref[2 * t : 3 * t] = (POST_DECAY * q2 + f2) * alive
    base_ref[0:t] = alive
    base_ref[t : 2 * t] = LEAK * LEAK * potential_ref[...] * alive
    fq_ref[...] = RATE * jnp.concatenate([f1, -q1], 0)
    factor = RATE * jnp.concatenate([-q1, f2 - q2, f1 + PRE_DECAY * f2], 0)
    fh = factor.astype(BF16).astype(F32)
    pad = left_ref.shape[1] - 9 * t
    left = jnp.concatenate([fh, fh, factor - fh, jnp.zeros((pad, n), F32)], 0)
    left_ref[...] = left.T.astype(BF16)

    @pl.loop(0, tiles)
    def _(c):
        w = w_ref[:, cols_of(c, block)]
        win[c] = w
        hi, lo = split(w)
        wsp[c, 0:block] = hi.T
        wsp[c, block : 2 * block] = lo.T


def mid_kernel(which_ref, *refs):
    areas, inner = which_ref.shape
    shared, outs = refs[:inner], refs[inner:]
    block = outs[0].shape[-1]
    area = lax.axis_index("area")
    for h in range(1, areas):
        to = partner(area, h, areas)[1]
        for k in range(inner):
            start = pl.multiple_of(which_ref[to, k] * block, block)
            outs[h - 1][k] = shared[k][:, pl.ds(start, block)]


def cols_of(c, block):
    return pl.ds(pl.multiple_of(c * block, block), block)


def update_terms(z):
    zh = z.astype(BF16).astype(F32)
    pad = jnp.zeros((z.shape[0] // 3, z.shape[1]), F32)
    return jnp.concatenate([zh, z - zh, zh, pad], 0).astype(BF16)


def current_terms(z, t):
    a1, a2, p1 = z[0:t], z[t : 2 * t], z[2 * t : 3 * t]
    rows = jnp.concatenate([LEAK * a1 + a2, a2], 0)
    rh = rows.astype(BF16).astype(F32)
    rl = rows - rh
    drive = jnp.concatenate([rh[0:t], rl[0:t]], 0).astype(BF16)
    late = jnp.concatenate([rh[t : 2 * t], rl[t : 2 * t]], 0).astype(BF16)
    th, tl = split(jnp.concatenate([p1, a1], 0))
    return (
        jnp.concatenate([drive, drive], 1),
        jnp.concatenate([late, late], 1),
        jnp.concatenate([th, tl], 1),
    )


def dot_nt(x, y):
    return lax.dot_general(x, y, NT, preferred_element_type=F32)


def near_kernel(left_ref, ends_ref, w_ref, *refs):
    inner = len(refs) - 9
    shared = refs[:inner]
    new_hbm, *end_hbm, sum_ref, gram_ref, wout, osem, esem = refs[inner:]
    t = sum_ref.shape[0] // 2
    tiles, n, block = wout.shape
    z = lax.axis_index("inarea")
    per = tiles // inner

    def flush(c):
        return pltpu.make_async_copy(wout.at[c], new_hbm.at[:, cols_of(c, block)], osem.at[c])

    def tile_of(k, h):
        return partner(z, k, inner)[0] * per + h

    ends = [
        pltpu.make_async_copy(ends_ref.at[i * t : (i + 1) * t], ref, esem.at[i])
        for i, ref in enumerate(end_hbm)
    ]
    for copy in ends:
        copy.start()
    total, gram = jnp.zeros(sum_ref.shape, F32), jnp.zeros(gram_ref.shape, F32)
    for k in range(inner):
        for h in range(per):
            c = tile_of(k, h)
            w = w_ref[:, cols_of(c, block)]
            x = shared[k][:, h * block : (h + 1) * block]
            drive, late, traces = current_terms(x, t)
            total = total + dot_nt(drive, jnp.concatenate(split(w), 1))
            gram = gram + dot_nt(late, traces)
            wout[c] = w + jnp.dot(
                left_ref[:, 0 : 10 * t], update_terms(x), preferred_element_type=F32)
            flush(c).start()
    sum_ref[...] = total
    gram_ref[...] = gram

    for c in range(tiles):
        flush(c).wait()
    for copy in ends:
        copy.wait()


def far_tiles(lo, hi, areas, slot_ref, left_ref, win, wsp, blocks, new_hbm, far_ref, wout, osem,
              total, gram):
    t = total.shape[0] // 2
    block = win.shape[2]
    area = lax.axis_index("area")

    def flush(c):
        return pltpu.make_async_copy(wout.at[c], new_hbm.at[:, cols_of(c, block)], osem.at[c])

    for h, ref in blocks:
        far_ref[partner(area, h, areas)[0]] = ref[...]

    def group(places):
        parts, grams = [], []
        for i in places:
            c = slot_ref[2, i]
            z = far_ref[slot_ref[0, i], slot_ref[1, i]]
            wout[c] = win[c] + jnp.dot(
                left_ref[:, 0 : 10 * t], update_terms(z), preferred_element_type=F32)
            flush(c).start()
        for i in places:
            c = slot_ref[2, i]
            drive, late, traces = current_terms(far_ref[slot_ref[0, i], slot_ref[1, i]], t)
            parts.append(jnp.dot(drive, wsp[c], preferred_element_type=F32))
            grams.append(dot_nt(late, traces))
        total[...] += sum(parts)
        gram[...] += sum(grams)

    quads = lax.div(hi - lo, 4)

    @pl.loop(0, quads)
    def _(i):
        group([lo + 4 * i + j for j in range(4)])

    rest = hi - lo - 4 * quads

    @pl.when(rest >= 2)
    def _():
        group((lo + 4 * quads, lo + 4 * quads + 1))

    @pl.when(lax.rem(rest, 2) == 1)
    def _():
        group((hi - 1,))

    def drain():
        @pl.loop(lo, hi)
        def _(i):
            flush(slot_ref[2, i]).wait()

    return drain


def early_kernel(areas, slot_ref, left_ref, sum_ref, gram_ref, win, wsp, *refs):
    *fars, new_hbm, total, gram, wout, far_ref, osem = refs
    total[...] = sum_ref[...]
    gram[...] = gram_ref[...]
    order, count = area_order(areas)
    blocks = list(zip(order[:count], fars, strict=True))
    far_tiles(0, slot_ref[3, 0], areas, slot_ref, left_ref, win, wsp, blocks, new_hbm, far_ref,
              wout, osem, total, gram)()


def late_kernel(areas, slot_ref, base_ref, fq_ref, left_ref, sum_ref, gram_ref, win, wsp, *refs):
    *fars, _, new_hbm, voltage_hbm, total, gram, wout, vout, far_ref, osem, vsem = refs
    t = vout.shape[0]
    total[...] = sum_ref[...]
    gram[...] = gram_ref[...]
    order, count = area_order(areas)
    blocks = list(zip(order[count:], fars, strict=True))
    drain = far_tiles(slot_ref[3, 0], win.shape[0], areas, slot_ref, left_ref, win, wsp, blocks,
                      new_hbm, far_ref, wout, osem, total, gram)
    pairs = gram[0:t] + gram[t : 2 * t]
    drift = jnp.dot(pairs, fq_ref[...], precision=lax.Precision.HIGHEST, preferred_element_type=F32)
    vout[...] = base_ref[t : 2 * t] + base_ref[0:t] * (total[0:t] + total[t : 2 * t] + drift)
    done = pltpu.make_async_copy(vout, voltage_hbm, vsem)
    done.start()
    drain()
    done.wait()


def full(space):
    return pl.BlockSpec(memory_space=space)


def local(spikes, release, potential, pre_trace, post_trace, w_local, w_long, sources, counts):
    t, n = release.shape
    slots = sources.shape[1]
    block = w_long.shape[1] // slots
    per_dev = n // block
    areas = lax.axis_size("area")
    inner = lax.axis_size("inarea")
    tiles = w_local.shape[1] // block
    cover = pl.CostEstimate(flops=5 * 10**9, bytes_accessed=1 << 24, transcendentals=0)

    def hb(*xs):
        return [pltpu.with_memory_space_constraint(x, HB) for x in xs]

    def vm(*xs):
        return [pltpu.with_memory_space_constraint(x, VM) for x in xs]

    def params(mib):
        return pltpu.CompilerParams(vmem_limit_bytes=mib << 20)

    pay, keep, held = pl.pallas_call(
        pre_kernel,
        out_shape=(
            VM((3 * t, n), F32), VM((4 * t, n), F32), SM(sources.shape, jnp.int32)),
        in_specs=[full(SM)] * 2 + [full(VM)] * 3,
        out_specs=(full(VM),) * 2 + (full(SM),),
        compiler_params=params(2),
        cost_estimate=cover,
        name="pre",
    )(*hb(counts, sources, spikes, release, pre_trace))

    shared = [pay] + [
        exchange(pay, "inarea", k) for k in range(1, inner)
    ]

    which, slot, left, fq, base, ends, tiles_w, halves_w = pl.pallas_call(
        functools.partial(prep_kernel, per_dev),
        out_shape=(
            SM((areas, inner), jnp.int32),
            SM((4, slots), jnp.int32),
            VM((n, 128), BF16),
            VM((2 * t, n), F32),
            VM((2 * t, n), F32),
            VM((3 * t, n), F32),
            VM((slots, n, block), F32),
            VM((slots, 2 * block, n), BF16),
        ),
        in_specs=[full(SM)] + [full(VM)] * 3 + [full(HB)] * 2,
        out_specs=(full(SM),) * 2 + (full(VM),) * 6,
        scratch_shapes=[
            VM((t, n), F32),
            VM((t, n), F32),
            pltpu.SemaphoreType.DMA((2,)),
        ],
        compiler_params=params(4),
        cost_estimate=pl.CostEstimate(
            flops=2 * n * w_long.shape[1] * 512, bytes_accessed=8 * w_long.size, transcendentals=0),
        name="prep",
    )(held, *vm(pay, keep, w_long), *hb(post_trace, potential))

    sends = pl.pallas_call(
        mid_kernel,
        out_shape=(VM((inner, 3 * t, block), F32),) * (areas - 1),
        in_specs=[full(SM)] + [full(VM)] * inner,
        out_specs=(full(VM),) * (areas - 1),
        compiler_params=params(2 + areas * inner * 12 * t * block // (1 << 20)),
        cost_estimate=cover,
        name="mid",
    )(which, *shared)
    order, count = area_order(areas)
    fars = [exchange(sends[h - 1], "area", h) for h in order]

    local_new, volley, presyn, postsyn, sums, grams = pl.pallas_call(
        near_kernel,
        out_shape=(
            HB(w_local.shape, F32),
            *(HB((t, n), F32),) * 3,
            VM((2 * t, n), F32),
            VM((2 * t, 2 * t), F32),
        ),
        in_specs=[full(VM)] * (3 + inner),
        out_specs=(full(HB),) * 4 + (full(VM),) * 2,
        scratch_shapes=[
            VM((tiles, n, block), F32),
            pltpu.SemaphoreType.DMA((tiles,)),
            pltpu.SemaphoreType.DMA((3,)),
        ],
        compiler_params=params(14),
        cost_estimate=pl.CostEstimate(
            flops=2 * n * w_local.shape[1] * 512, bytes_accessed=8 * w_local.size, transcendentals=0),
        name="near",
    )(*vm(left, ends, w_local), *shared)

    far_scratch = [
        VM((slots, n, block), F32),
        VM((areas, inner, 3 * t, block), F32),
        pltpu.SemaphoreType.DMA((slots,)),
    ]
    far_params = params(12 + areas * inner * 12 * t * block // (1 << 20))
    far_cost = pl.CostEstimate(
        flops=n * w_long.shape[1] * 512, bytes_accessed=4 * w_long.size, transcendentals=0)
    soon, then = fars[:count], fars[count:]
    long_new, sums, grams = pl.pallas_call(
        functools.partial(early_kernel, areas),
        out_shape=(HB(w_long.shape, F32), VM((2 * t, n), F32), VM((2 * t, 2 * t), F32)),
        in_specs=[full(SM)] + [full(VM)] * (5 + len(soon)),
        out_specs=(full(HB), full(VM), full(VM)),
        scratch_shapes=far_scratch,
        compiler_params=far_params,
        cost_estimate=far_cost,
        name="early",
    )(slot, *vm(left, sums, grams, tiles_w, halves_w), *soon)

    long_new, voltage = pl.pallas_call(
        functools.partial(late_kernel, areas),
        out_shape=(HB(w_long.shape, F32), HB((t, n), F32)),
        in_specs=[full(SM)] + [full(VM)] * (7 + len(then)) + [full(HB)],
        out_specs=(full(HB),) * 2,
        scratch_shapes=[VM((2 * t, n), F32), VM((2 * t, 2 * t), F32), far_scratch[0], VM((t, n), F32)]
        + far_scratch[1:] + [pltpu.SemaphoreType.DMA],
        input_output_aliases={8 + len(then): 0},
        compiler_params=far_params,
        cost_estimate=far_cost,
        name="late",
    )(slot, *vm(base, fq, left, sums, grams, tiles_w, halves_w), *then, *hb(long_new))
    return voltage, volley, presyn, postsyn, local_new, long_new


def solution(mesh):
    split_last = P(None, ("area", "inarea"))
    rows = P(("area", "inarea"), None)
    return jax.shard_map(
        local,
        mesh=mesh,
        in_specs=(
            P(None, None, ("area", "inarea")),
            split_last, split_last, split_last, split_last, rows, rows, P(), P(),
        ),
        out_specs=(split_last, split_last, split_last, split_last, rows, rows),
        check_vma=False,
    )
```

```python
import functools

import jax
import jax.numpy as jnp
from jax import lax
from jax.experimental import pallas as pl
from jax.experimental.pallas import tpu as pltpu
from jax.sharding import PartitionSpec as P

PRE_DECAY = 0.8
POST_DECAY = 0.7
LEAK = 0.9
RATE = 0.0005
RECOVERY = 0.2
DEPLETION = 0.5

F32 = jnp.float32
BF16 = jnp.bfloat16
NT = (((1,), (1,)), ((), ()))
VM = pltpu.VMEM
SM = pltpu.SMEM
HB = pltpu.HBM
AORDER = (6, 4, 2, 1, 7, 5, 3)
EARLY = 4


def partner(i, k, size):
    if size & (size - 1) == 0:
        return i ^ k, i ^ k
    return (i + size - k) % size, (i + k) % size


def sender_of(src, i, size):
    if size & (size - 1) == 0:
        return src ^ i
    return (i + size - src) % size


def area_order(size):
    if size == 8:
        return AORDER, EARLY
    return tuple(range(1, size)), size // 2


def is_early(k, size):
    order, count = area_order(size)
    early = k == order[0]
    for h in order[1:count]:
        early = early | (k == h)
    return early


def exchange(x, axis, k):
    size = lax.axis_size(axis)
    return lax.ppermute(x, axis, [(i, partner(i, k, size)[1]) for i in range(size)])


def alive_mask(counts_ref, shape):
    live = counts_ref[lax.axis_index("area")] - lax.axis_index("inarea") * shape[-1]
    return (lax.broadcasted_iota(jnp.int32, shape, len(shape) - 1) < live).astype(F32)


def split(x):
    hi = x.astype(BF16)
    return hi, (x - hi.astype(F32)).astype(BF16)


def pre_kernel(
    counts_ref, sources_ref, spikes_ref, release_ref, pre_ref, pay_ref, keep_ref, held_ref
):
    t = release_ref.shape[0]
    alive = alive_mask(counts_ref, release_ref.shape)
    f1 = spikes_ref[0].astype(F32) * alive
    f2 = spikes_ref[1].astype(F32) * alive
    v1 = release_ref[...]
    a1 = f1 * v1
    v2 = v1 + RECOVERY * (1.0 - v1) - DEPLETION * a1
    pay_ref[0:t] = a1
    pay_ref[t : 2 * t] = f2 * v2
    pay_ref[2 * t : 3 * t] = (PRE_DECAY * pre_ref[...] + a1) * alive
    for i, part in enumerate((f1, f2, v2, alive)):
        keep_ref[i * t : (i + 1) * t] = part
    for b in range(sources_ref.shape[0]):
        for c in range(sources_ref.shape[1]):
            held_ref[b, c] = sources_ref[b, c]


def prep_kernel(
    per_dev, sources_ref, pay_ref, keep_ref, w_ref, post_hbm, potential_hbm,
    which_ref, slot_ref, left_ref, fq_ref, base_ref, ends_ref, win, wsp,
    post_ref, potential_ref, msem,
):
    t, n = post_ref.shape
    tiles, _, block = win.shape
    areas, inner = which_ref.shape
    slots = sources_ref.shape[1]
    area, z = lax.axis_index("area"), lax.axis_index("inarea")

    small = [
        pltpu.make_async_copy(post_hbm, post_ref, msem.at[0]),
        pltpu.make_async_copy(potential_hbm, potential_ref, msem.at[1]),
    ]
    for copy in small:
        copy.start()

    for k in range(inner):
        first = (area * inner + partner(z, k, inner)[0]) * per_dev

        @pl.loop(0, areas)
        def _(b):
            which = jnp.int32(0)
            for s in range(slots):
                off = sources_ref[b, s] - first
                which = which + jnp.where((off >= 0) & (off < per_dev), off, 0)
            which_ref[b, k] = which

    first, last = jnp.int32(0), jnp.int32(slots - 1)
    for s in range(slots):
        dev = lax.div(sources_ref[area, s], per_dev)
        origin = lax.div(dev, inner)
        early = is_early(sender_of(origin, area, areas), areas)
        at = jnp.where(early, first, last)
        slot_ref[0, at] = origin
        slot_ref[1, at] = sender_of(lax.rem(dev, inner), z, inner)
        slot_ref[2, at] = jnp.int32(s)
        first = first + jnp.where(early, 1, 0)
        last = last - jnp.where(early, 0, 1)
    slot_ref[3, 0] = first

    for copy in small:
        copy.wait()
    f1, f2, v2, alive = (keep_ref[i * t : (i + 1) * t] for i in range(4))
    a2, p1 = pay_ref[t : 2 * t], pay_ref[2 * t : 3 * t]
    q1 = post_ref[...]
    q2 = (POST_DECAY * q1 + f1) * alive
    ends_ref[0:t] = v2 + RECOVERY * (1.0 - v2) - DEPLETION * a2
    ends_ref[t : 2 * t] = (PRE_DECAY * p1 + a2) * alive
    ends_ref[2 * t : 3 * t] = (POST_DECAY * q2 + f2) * alive
    base_ref[0:t] = alive
    base_ref[t : 2 * t] = LEAK * LEAK * potential_ref[...] * alive
    fq_ref[...] = RATE * jnp.concatenate([f1, -q1], 0)
    factor = RATE * jnp.concatenate([-q1, f2 - q2, f1 + PRE_DECAY * f2], 0)
    fh = factor.astype(BF16).astype(F32)
    pad = left_ref.shape[1] - 9 * t
    left = jnp.concatenate([fh, fh, factor - fh, jnp.zeros((pad, n), F32)], 0)
    left_ref[...] = left.T.astype(BF16)

    @pl.loop(0, tiles)
    def _(c):
        w = w_ref[:, cols_of(c, block)]
        win[c] = w
        hi, lo = split(w)
        wsp[c, 0:block] = hi.T
        wsp[c, block : 2 * block] = lo.T


def mid_kernel(which_ref, *refs):
    areas, inner = which_ref.shape
    shared, outs = refs[:inner], refs[inner:]
    block = outs[0].shape[-1]
    area = lax.axis_index("area")
    for h in range(1, areas):
        to = partner(area, h, areas)[1]
        for k in range(inner):
            start = pl.multiple_of(which_ref[to, k] * block, block)
            outs[h - 1][k] = shared[k][:, pl.ds(start, block)]


def cols_of(c, block):
    return pl.ds(pl.multiple_of(c * block, block), block)


def update_terms(z):
    zh = z.astype(BF16).astype(F32)
    pad = jnp.zeros((z.shape[0] // 3, z.shape[1]), F32)
    return jnp.concatenate([zh, z - zh, zh, pad], 0).astype(BF16)


def current_terms(z, t):
    a1, a2, p1 = z[0:t], z[t : 2 * t], z[2 * t : 3 * t]
    rows = jnp.concatenate([LEAK * a1 + a2, a2], 0)
    rh = rows.astype(BF16).astype(F32)
    rl = rows - rh
    drive = jnp.concatenate([rh[0:t], rl[0:t]], 0).astype(BF16)
    late = jnp.concatenate([rh[t : 2 * t], rl[t : 2 * t]], 0).astype(BF16)
    th, tl = split(jnp.concatenate([p1, a1], 0))
    return (
        jnp.concatenate([drive, drive], 1),
        jnp.concatenate([late, late], 1),
        jnp.concatenate([th, tl], 1),
    )


def dot_nt(x, y):
    return lax.dot_general(x, y, NT, preferred_element_type=F32)


def near_kernel(left_ref, ends_ref, w_ref, *refs):
    inner = len(refs) - 9
    shared = refs[:inner]
    new_hbm, *end_hbm, sum_ref, gram_ref, wout, osem, esem = refs[inner:]
    t = sum_ref.shape[0] // 2
    tiles, n, block = wout.shape
    z = lax.axis_index("inarea")
    per = tiles // inner

    def flush(c):
        return pltpu.make_async_copy(wout.at[c], new_hbm.at[:, cols_of(c, block)], osem.at[c])

    def tile_of(k, h):
        return partner(z, k, inner)[0] * per + h

    ends = [
        pltpu.make_async_copy(ends_ref.at[i * t : (i + 1) * t], ref, esem.at[i])
        for i, ref in enumerate(end_hbm)
    ]
    for copy in ends:
        copy.start()
    total, gram = jnp.zeros(sum_ref.shape, F32), jnp.zeros(gram_ref.shape, F32)
    for k in range(inner):
        for h in range(per):
            c = tile_of(k, h)
            w = w_ref[:, cols_of(c, block)]
            x = shared[k][:, h * block : (h + 1) * block]
            drive, late, traces = current_terms(x, t)
            total = total + dot_nt(drive, jnp.concatenate(split(w), 1))
            gram = gram + dot_nt(late, traces)
            wout[c] = w + jnp.dot(
                left_ref[:, 0 : 10 * t], update_terms(x), preferred_element_type=F32)
            flush(c).start()
    sum_ref[...] = total
    gram_ref[...] = gram

    for c in range(tiles):
        flush(c).wait()
    for copy in ends:
        copy.wait()


def far_tiles(lo, hi, areas, slot_ref, left_ref, win, wsp, blocks, new_hbm, far_ref, wout, osem,
              total, gram):
    t = total.shape[0] // 2
    block = win.shape[2]
    area = lax.axis_index("area")

    def flush(c):
        return pltpu.make_async_copy(wout.at[c], new_hbm.at[:, cols_of(c, block)], osem.at[c])

    for h, ref in blocks:
        far_ref[partner(area, h, areas)[0]] = ref[...]

    def group(places):
        parts, grams = [], []
        for i in places:
            c = slot_ref[2, i]
            z = far_ref[slot_ref[0, i], slot_ref[1, i]]
            wout[c] = win[c] + jnp.dot(
                left_ref[:, 0 : 10 * t], update_terms(z), preferred_element_type=F32)
            flush(c).start()
        for i in places:
            c = slot_ref[2, i]
            drive, late, traces = current_terms(far_ref[slot_ref[0, i], slot_ref[1, i]], t)
            parts.append(jnp.dot(drive, wsp[c], preferred_element_type=F32))
            grams.append(dot_nt(late, traces))
        total[...] += sum(parts)
        gram[...] += sum(grams)

    quads = lax.div(hi - lo, 4)

    @pl.loop(0, quads)
    def _(i):
        group([lo + 4 * i + j for j in range(4)])

    rest = hi - lo - 4 * quads

    @pl.when(rest >= 2)
    def _():
        group((lo + 4 * quads, lo + 4 * quads + 1))

    @pl.when(lax.rem(rest, 2) == 1)
    def _():
        group((hi - 1,))

    def drain():
        @pl.loop(lo, hi)
        def _(i):
            flush(slot_ref[2, i]).wait()

    return drain


def early_kernel(areas, slot_ref, left_ref, sum_ref, gram_ref, win, wsp, *refs):
    *fars, new_hbm, total, gram, wout, far_ref, osem = refs
    total[...] = sum_ref[...]
    gram[...] = gram_ref[...]
    order, count = area_order(areas)
    blocks = list(zip(order[:count], fars, strict=True))
    far_tiles(0, slot_ref[3, 0], areas, slot_ref, left_ref, win, wsp, blocks, new_hbm, far_ref,
              wout, osem, total, gram)()


def late_kernel(areas, slot_ref, base_ref, fq_ref, left_ref, sum_ref, gram_ref, win, wsp, *refs):
    *fars, _, new_hbm, voltage_hbm, total, gram, wout, vout, far_ref, osem, vsem = refs
    t = vout.shape[0]
    total[...] = sum_ref[...]
    gram[...] = gram_ref[...]
    order, count = area_order(areas)
    blocks = list(zip(order[count:], fars, strict=True))
    drain = far_tiles(slot_ref[3, 0], win.shape[0], areas, slot_ref, left_ref, win, wsp, blocks,
                      new_hbm, far_ref, wout, osem, total, gram)
    pairs = gram[0:t] + gram[t : 2 * t]
    (ph, pq), (fh, fq) = split(pairs), split(fq_ref[...])
    drift = sum(jnp.dot(x, y, preferred_element_type=F32) for x, y in ((ph, fh), (ph, fq), (pq, fh)))
    vout[...] = base_ref[t : 2 * t] + base_ref[0:t] * (total[0:t] + total[t : 2 * t] + drift)
    done = pltpu.make_async_copy(vout, voltage_hbm, vsem)
    done.start()
    drain()
    done.wait()


def full(space):
    return pl.BlockSpec(memory_space=space)


def local(spikes, release, potential, pre_trace, post_trace, w_local, w_long, sources, counts):
    t, n = release.shape
    slots = sources.shape[1]
    block = w_long.shape[1] // slots
    per_dev = n // block
    areas = lax.axis_size("area")
    inner = lax.axis_size("inarea")
    tiles = w_local.shape[1] // block
    cover = pl.CostEstimate(flops=5 * 10**9, bytes_accessed=1 << 24, transcendentals=0)

    def hb(*xs):
        return [pltpu.with_memory_space_constraint(x, HB) for x in xs]

    def vm(*xs):
        return [pltpu.with_memory_space_constraint(x, VM) for x in xs]

    def params(mib):
        return pltpu.CompilerParams(vmem_limit_bytes=mib << 20)

    pay, keep, held = pl.pallas_call(
        pre_kernel,
        out_shape=(
            VM((3 * t, n), F32), VM((4 * t, n), F32), SM(sources.shape, jnp.int32)),
        in_specs=[full(SM)] * 2 + [full(VM)] * 3,
        out_specs=(full(VM),) * 2 + (full(SM),),
        compiler_params=params(2),
        cost_estimate=cover,
        name="pre",
    )(*hb(counts, sources, spikes, release, pre_trace))

    shared = [pay] + [
        exchange(pay, "inarea", k) for k in range(1, inner)
    ]

    which, slot, left, fq, base, ends, tiles_w, halves_w = pl.pallas_call(
        functools.partial(prep_kernel, per_dev),
        out_shape=(
            SM((areas, inner), jnp.int32),
            SM((4, slots), jnp.int32),
            VM((n, 128), BF16),
            VM((2 * t, n), F32),
            VM((2 * t, n), F32),
            VM((3 * t, n), F32),
            VM((slots, n, block), F32),
            VM((slots, 2 * block, n), BF16),
        ),
        in_specs=[full(SM)] + [full(VM)] * 3 + [full(HB)] * 2,
        out_specs=(full(SM),) * 2 + (full(VM),) * 6,
        scratch_shapes=[
            VM((t, n), F32),
            VM((t, n), F32),
            pltpu.SemaphoreType.DMA((2,)),
        ],
        compiler_params=params(4),
        cost_estimate=pl.CostEstimate(
            flops=2 * n * w_long.shape[1] * 512, bytes_accessed=8 * w_long.size, transcendentals=0),
        name="prep",
    )(held, *vm(pay, keep, w_long), *hb(post_trace, potential))

    sends = pl.pallas_call(
        mid_kernel,
        out_shape=(VM((inner, 3 * t, block), F32),) * (areas - 1),
        in_specs=[full(SM)] + [full(VM)] * inner,
        out_specs=(full(VM),) * (areas - 1),
        compiler_params=params(2 + areas * inner * 12 * t * block // (1 << 20)),
        cost_estimate=cover,
        name="mid",
    )(which, *shared)
    order, count = area_order(areas)
    fars = [exchange(sends[h - 1], "area", h) for h in order]

    local_new, volley, presyn, postsyn, sums, grams = pl.pallas_call(
        near_kernel,
        out_shape=(
            HB(w_local.shape, F32),
            *(HB((t, n), F32),) * 3,
            VM((2 * t, n), F32),
            VM((2 * t, 2 * t), F32),
        ),
        in_specs=[full(VM)] * (3 + inner),
        out_specs=(full(HB),) * 4 + (full(VM),) * 2,
        scratch_shapes=[
            VM((tiles, n, block), F32),
            pltpu.SemaphoreType.DMA((tiles,)),
            pltpu.SemaphoreType.DMA((3,)),
        ],
        compiler_params=params(14),
        cost_estimate=pl.CostEstimate(
            flops=2 * n * w_local.shape[1] * 512, bytes_accessed=8 * w_local.size, transcendentals=0),
        name="near",
    )(*vm(left, ends, w_local), *shared)

    far_scratch = [
        VM((slots, n, block), F32),
        VM((areas, inner, 3 * t, block), F32),
        pltpu.SemaphoreType.DMA((slots,)),
    ]
    far_params = params(12 + areas * inner * 12 * t * block // (1 << 20))
    far_cost = pl.CostEstimate(
        flops=n * w_long.shape[1] * 512, bytes_accessed=4 * w_long.size, transcendentals=0)
    soon, then = fars[:count], fars[count:]
    long_new, sums, grams = pl.pallas_call(
        functools.partial(early_kernel, areas),
        out_shape=(HB(w_long.shape, F32), VM((2 * t, n), F32), VM((2 * t, 2 * t), F32)),
        in_specs=[full(SM)] + [full(VM)] * (5 + len(soon)),
        out_specs=(full(HB), full(VM), full(VM)),
        scratch_shapes=far_scratch,
        compiler_params=far_params,
        cost_estimate=far_cost,
        name="early",
    )(slot, *vm(left, sums, grams, tiles_w, halves_w), *soon)

    long_new, voltage = pl.pallas_call(
        functools.partial(late_kernel, areas),
        out_shape=(HB(w_long.shape, F32), HB((t, n), F32)),
        in_specs=[full(SM)] + [full(VM)] * (7 + len(then)) + [full(HB)],
        out_specs=(full(HB),) * 2,
        scratch_shapes=[VM((2 * t, n), F32), VM((2 * t, 2 * t), F32), far_scratch[0], VM((t, n), F32)]
        + far_scratch[1:] + [pltpu.SemaphoreType.DMA],
        input_output_aliases={8 + len(then): 0},
        compiler_params=far_params,
        cost_estimate=far_cost,
        name="late",
    )(slot, *vm(base, fq, left, sums, grams, tiles_w, halves_w), *then, *hb(long_new))
    return voltage, volley, presyn, postsyn, local_new, long_new


def solution(mesh):
    split_last = P(None, ("area", "inarea"))
    rows = P(("area", "inarea"), None)
    return jax.shard_map(
        local,
        mesh=mesh,
        in_specs=(
            P(None, None, ("area", "inarea")),
            split_last, split_last, split_last, split_last, rows, rows, P(), P(),
        ),
        out_specs=(split_last, split_last, split_last, split_last, rows, rows),
        check_vma=False,
    )
```
